32 devices in a mesh: dp: 8 (over z, x), row: 2 (over y), col: 2 (over core).
Axes of the slice: x: 2, y: 2, z: 4, core: 2. Of those that a mesh axis runs over, the one named last changes fastest.
Arguments:
- activations: bfloat16 [8192, 2048], P('dp', ('row', 'col')), may hold values from -0.08984375 to 0.08984375
- gate_input: bfloat16 [8192, 5120], P('dp', ('row', 'col')), may hold values from -6 to 6
- up_input: bfloat16 [8192, 5120], P('dp', ('row', 'col')), may hold values from -6 to 6
- hidden_grad: bfloat16 [8192, 5120], P('dp', ('row', 'col')), may hold values from -6 to 6
- weight_gate: bfloat16 [2048, 5120], P(None, ('row', 'col')), may hold values from -0.125 to 0.125
- weight_up: bfloat16 [2048, 5120], P(None, ('row', 'col')), may hold values from -0.125 to 0.125
Outputs:
- input_grad: float32 [8192, 2048], P('dp', ('row', 'col'))
- gate_weight_grad: float32 [2048, 5120], P(None, ('row', 'col'))
- up_weight_grad: float32 [2048, 5120], P(None, ('row', 'col'))
The draws below stay inside these ranges and needn't reach their ends.
All inputs are finite; a program needn't handle non-finite values.
Results may differ from the reference program's by a relative error of at most 0.0029.
Values may be sent and summed in bfloat16 or wider, within the bound.
A program may use at most 128 MiB of HBM per device.

```python
import jax
import jax.numpy as jnp
from jax import lax

D = 2048
FF = 5120
TOKENS = 8192


def levels(own_key, shape, cuts, smallest, largest):
    def one(position, parts):
        draws = jax.random.uniform(jax.random.fold_in(jax.random.fold_in(own_key, 6), position), (parts,), jnp.float32, smallest / len(cuts), largest / len(cuts))
        return jnp.repeat(jnp.exp(draws), shape[position] // parts).reshape((-1,) + (1,) * (len(shape) - position - 1))

    loudness = one(*cuts[0])
    for cut in cuts[1:]:
        loudness = loudness * one(*cut)
    return loudness


def bell_draw(own_key, shape, spread, most, cuts=(), dtype=jnp.bfloat16):
    entries = spread * jax.random.normal(own_key, shape, jnp.float32)
    if cuts:
        entries = entries * levels(own_key, shape, cuts, -0.22, 0.18)
    return jnp.clip(entries, -most, most).astype(dtype)


def setup_inputs(seed: int = 0) -> dict:
    streams_of = jax.random.split(jax.random.key(seed), 7)
    activations = bell_draw(streams_of[0], (TOKENS, D), 0.015, 0.08984375, ((0, 8), (1, 4)))
    gate_input = bell_draw(streams_of[1], (TOKENS, FF), 1.0, 6.0, ((0, 8), (1, 4)))
    up_input = bell_draw(streams_of[2], (TOKENS, FF), 1.0, 6.0, ((0, 8), (1, 4)))
    hidden_grad = bell_draw(streams_of[3], (TOKENS, FF), 1.0, 6.0, ((0, 8), (1, 4)))
    weight_gate = bell_draw(streams_of[4], (D, FF), D ** -0.5, 0.125, ((1, 4),))
    weight_up = bell_draw(streams_of[5], (D, FF), D ** -0.5, 0.125, ((1, 4),))
    return dict(activations=activations, gate_input=gate_input, up_input=up_input, hidden_grad=hidden_grad, weight_gate=weight_gate, weight_up=weight_up)


ROOT_TWO_PI = 0.7978845608028654
CUBIC = 0.044715


def reference(activations, gate_input, up_input, hidden_grad, weight_gate, weight_up):
    gate_pre = gate_input.astype(jnp.float32)
    up_pre = up_input.astype(jnp.float32)
    grad_hidden = hidden_grad.astype(jnp.float32)
    tanh_part = jnp.tanh(ROOT_TWO_PI * (gate_pre + CUBIC * gate_pre * gate_pre * gate_pre))
    gelu_value = 0.5 * gate_pre * (1.0 + tanh_part)
    gelu_slope = 0.5 * (1.0 + tanh_part) + 0.5 * gate_pre * (1.0 - tanh_part * tanh_part) * ROOT_TWO_PI * (1.0 + 3.0 * CUBIC * gate_pre * gate_pre)
    gate_grad = (grad_hidden * up_pre * gelu_slope).astype(jnp.bfloat16)
    up_grad = (grad_hidden * gelu_value).astype(jnp.bfloat16)
    dims_feature = (((1,), (1,)), ((), ()))
    dims_tokens = (((0,), (0,)), ((), ()))
    input_grad = lax.dot_general(gate_grad, weight_gate, dims_feature, preferred_element_type=jnp.float32)
    input_grad = input_grad + lax.dot_general(up_grad, weight_up, dims_feature, preferred_element_type=jnp.float32)
    gate_weight_grad = lax.dot_general(activations, gate_grad, dims_tokens, preferred_element_type=jnp.float32)
    up_weight_grad = lax.dot_general(activations, up_grad, dims_tokens, preferred_element_type=jnp.float32)
    return input_grad.astype(jnp.float32), gate_weight_grad, up_weight_grad
```

```python
import jax
import jax.numpy as jnp
from jax import lax
from jax.sharding import PartitionSpec as P

ROOT_TWO_PI = 0.7978845608028654
CUBIC = 0.044715


def geglu_grads(gate_input, up_input, hidden_grad):
    gate_pre = gate_input.astype(jnp.float32)
    up_pre = up_input.astype(jnp.float32)
    grad_hidden = hidden_grad.astype(jnp.float32)
    tanh_part = jnp.tanh(ROOT_TWO_PI * (gate_pre + CUBIC * gate_pre * gate_pre * gate_pre))
    gelu_value = 0.5 * gate_pre * (1.0 + tanh_part)
    gelu_slope = 0.5 * (1.0 + tanh_part) + 0.5 * gate_pre * (
        1.0 - tanh_part * tanh_part
    ) * ROOT_TWO_PI * (1.0 + 3.0 * CUBIC * gate_pre * gate_pre)
    gate_grad = (grad_hidden * up_pre * gelu_slope).astype(jnp.bfloat16)
    up_grad = (grad_hidden * gelu_value).astype(jnp.bfloat16)
    return (gate_grad, up_grad)


def contract_hidden(grad_rows, weight_rows):
    return lax.dot_general(
        grad_rows, weight_rows, (((1,), (1,)), ((), ())), preferred_element_type=jnp.float32
    )


def contract_tokens(act_rows, grad_rows):
    return lax.dot_general(
        act_rows, grad_rows, (((0,), (0,)), ((), ())), preferred_element_type=jnp.float32
    )


def narrow(value):
    return value.astype(jnp.bfloat16)


def wide(value):
    return value.astype(jnp.float32)


def ring_shift(value, axis, size, step):
    return lax.ppermute(value, axis, [(i, (i + step) % size) for i in range(size)])


def make_body(dp, rows, cols):
    outer = 4 if dp % 4 == 0 else 1
    inner = dp // outer

    def outer_shift(value, step):
        pairs = [
            (z * inner + x, ((z + step) % outer) * inner + x)
            for z in range(outer)
            for x in range(inner)
        ]
        return lax.ppermute(value, "dp", pairs)

    def inner_shift(value, step):
        pairs = [
            (z * inner + x, z * inner + (x + step) % inner)
            for z in range(outer)
            for x in range(inner)
        ]
        return lax.ppermute(value, "dp", pairs)

    def reduce_tokens(gathered, grad, turn):
        width = gathered.shape[1] // outer
        place = lax.axis_index("dp")
        z, x = place // inner, place % inner

        def part(step):
            start = ((z + turn * step) % outer) * width
            return contract_tokens(
                lax.dynamic_slice_in_dim(gathered, start, width, axis=1), grad
            )

        if outer == 4:
            relayed = outer_shift(narrow(part(2)), turn)
            backward = outer_shift(narrow(part(-1)), -turn)
            forward = outer_shift(narrow(part(1) + wide(relayed)), turn)
            total = part(0) + wide(backward) + wide(forward)
        else:
            total = part(0)
        depth = width // inner

        def piece(step):
            return lax.dynamic_slice_in_dim(
                total, ((x + step) % inner) * depth, depth, axis=0
            )

        summed = piece(0)
        for step in range(1, inner):
            summed = summed + wide(inner_shift(narrow(piece(step)), step))
        return narrow(summed)

    def reduce_hidden(gate_grad, up_grad, weight_gate, weight_up):
        width = weight_gate.shape[0] // (rows * cols)
        r, c = lax.axis_index("row"), lax.axis_index("col")

        def part(row_step, col_step):
            block = ((r + row_step) % rows) * cols + (c + col_step) % cols
            return contract_hidden(
                gate_grad, lax.dynamic_slice_in_dim(weight_gate, block * width, width, axis=0)
            ) + contract_hidden(
                up_grad, lax.dynamic_slice_in_dim(weight_up, block * width, width, axis=0)
            )

        def over_cols(row_step):
            moved = [
                ring_shift(narrow(part(row_step, step)), "col", cols, step)
                for step in range(1, cols)
            ]
            total = part(row_step, 0)
            for value in moved:
                total = total + wide(value)
            return total

        moved = [
            ring_shift(narrow(over_cols(step)), "row", rows, step) for step in range(1, rows)
        ]
        total = over_cols(0)
        for value in moved:
            total = total + wide(value)
        return total

    def body(activations, gate_input, up_input, hidden_grad, weight_gate, weight_up):
        gathered = lax.all_gather(activations, ("row", "col"), axis=1, tiled=True)
        gate_grad, up_grad = geglu_grads(gate_input, up_input, hidden_grad)
        gate_part = reduce_tokens(gathered, gate_grad, 1)
        up_part = reduce_tokens(gathered, up_grad, -1)
        gate_weight_grad = wide(lax.all_gather(gate_part, "dp", axis=0, tiled=True))
        up_weight_grad = wide(lax.all_gather(up_part, "dp", axis=0, tiled=True))
        input_grad = reduce_hidden(gate_grad, up_grad, weight_gate, weight_up)
        return (input_grad, gate_weight_grad, up_weight_grad)

    return body


def solution(mesh):
    in_specs = (
        P("dp", ("row", "col")),
        P("dp", ("row", "col")),
        P("dp", ("row", "col")),
        P("dp", ("row", "col")),
        P(None, ("row", "col")),
        P(None, ("row", "col")),
    )
    out_specs = (P("dp", ("row", "col")), P(None, ("row", "col")), P(None, ("row", "col")))
    body = make_body(mesh.shape["dp"], mesh.shape["row"], mesh.shape["col"])
    return jax.shard_map(body, mesh=mesh, in_specs=in_specs, out_specs=out_specs, check_vma=False)
```

```python
import jax
import jax.numpy as jnp
from jax import lax
from jax.sharding import PartitionSpec as P

ROOT_TWO_PI = 0.7978845608028654
CUBIC = 0.044715


def geglu_grads(gate_input, up_input, hidden_grad):
    gate_pre = gate_input.astype(jnp.float32)
    up_pre = up_input.astype(jnp.float32)
    grad_hidden = hidden_grad.astype(jnp.float32)
    tanh_part = jnp.tanh(ROOT_TWO_PI * (gate_pre + CUBIC * gate_pre * gate_pre * gate_pre))
    gelu_value = 0.5 * gate_pre * (1.0 + tanh_part)
    gelu_slope = 0.5 * (1.0 + tanh_part) + 0.5 * gate_pre * (
        1.0 - tanh_part * tanh_part
    ) * ROOT_TWO_PI * (1.0 + 3.0 * CUBIC * gate_pre * gate_pre)
    gate_grad = (grad_hidden * up_pre * gelu_slope).astype(jnp.bfloat16)
    up_grad = (grad_hidden * gelu_value).astype(jnp.bfloat16)
    return (gate_grad, up_grad)


def contract_hidden(grad_rows, weight_rows):
    return lax.dot_general(
        grad_rows, weight_rows, (((1,), (1,)), ((), ())), preferred_element_type=jnp.float32
    )


def contract_tokens(act_rows, grad_rows):
    return lax.dot_general(
        act_rows, grad_rows, (((0,), (0,)), ((), ())), preferred_element_type=jnp.float32
    )


def narrow(value):
    return value.astype(jnp.bfloat16)


def wide(value):
    return value.astype(jnp.float32)


def ring_shift(value, axis, size, step):
    return lax.ppermute(value, axis, [(i, (i + step) % size) for i in range(size)])


def make_body(dp, rows, cols):
    outer = 4 if dp % 4 == 0 else 1
    inner = dp // outer

    def outer_shift(value, step):
        pairs = [
            (z * inner + x, ((z + step) % outer) * inner + x)
            for z in range(outer)
            for x in range(inner)
        ]
        return lax.ppermute(value, "dp", pairs)

    def inner_shift(value, step):
        pairs = [
            (z * inner + x, z * inner + (x + step) % inner)
            for z in range(outer)
            for x in range(inner)
        ]
        return lax.ppermute(value, "dp", pairs)

    def reduce_tokens(gathered, grad, turn):
        width = gathered.shape[1] // outer
        place = lax.axis_index("dp")
        z, x = place // inner, place % inner

        def part(step):
            start = ((z + turn * step) % outer) * width
            return contract_tokens(
                lax.dynamic_slice_in_dim(gathered, start, width, axis=1), grad
            )

        if outer == 4:
            relayed = outer_shift(narrow(part(2)), turn)
            backward = outer_shift(narrow(part(-1)), -turn)
            relayed, backward = yield (relayed, backward)
            forward = outer_shift(narrow(part(1) + wide(relayed)), turn)
            (forward,) = yield (forward,)
            total = part(0) + wide(backward) + wide(forward)
        else:
            total = part(0)
        depth = width // inner

        def piece(step):
            return lax.dynamic_slice_in_dim(
                total, ((x + step) % inner) * depth, depth, axis=0
            )

        summed = piece(0)
        for step in range(1, inner):
            summed = summed + wide(inner_shift(narrow(piece(step)), step))
        yield narrow(summed)

    def spread_tokens(own, turn):
        depth = own.shape[0]
        width = depth * inner
        place = lax.axis_index("dp")
        z, x = place // inner, place % inner
        chunk = jnp.zeros((width, own.shape[1]), own.dtype)
        chunk = lax.dynamic_update_slice_in_dim(chunk, own, x * depth, axis=0)
        for step in range(1, inner):
            other = inner_shift(own, step)
            chunk = lax.dynamic_update_slice_in_dim(
                chunk, other, ((x - step) % inner) * depth, axis=0
            )
        if outer != 4:
            yield wide(chunk)
            return
        (chunk,) = yield (chunk,)
        near = outer_shift(chunk, turn)
        back = outer_shift(chunk, -turn)
        near, back = yield (near, back)
        far = outer_shift(near, turn)
        whole = jnp.zeros((outer * width, own.shape[1]), jnp.float32)
        for step, value in ((0, chunk), (-1, near), (1, back), (2, far)):
            start = ((z + turn * step) % outer) * width
            whole = lax.dynamic_update_slice_in_dim(whole, wide(value), start, axis=0)
        yield whole

    def reduce_hidden(gate_grad, up_grad, weight_gate, weight_up):
        width = weight_gate.shape[0] // (rows * cols)
        r, c = lax.axis_index("row"), lax.axis_index("col")

        def part(row_step, col_step):
            block = ((r + row_step) % rows) * cols + (c + col_step) % cols
            return contract_hidden(
                gate_grad, lax.dynamic_slice_in_dim(weight_gate, block * width, width, axis=0)
            ) + contract_hidden(
                up_grad, lax.dynamic_slice_in_dim(weight_up, block * width, width, axis=0)
            )

        def over_cols(row_step):
            moved = [
                ring_shift(narrow(part(row_step, step)), "col", cols, step)
                for step in range(1, cols)
            ]
            total = part(row_step, 0)
            for value in moved:
                total = total + wide(value)
            return total

        moved = [
            ring_shift(narrow(over_cols(step)), "row", rows, step) for step in range(1, rows)
        ]
        total = over_cols(0)
        for value in moved:
            total = total + wide(value)
        return total

    def body(activations, gate_input, up_input, hidden_grad, weight_gate, weight_up):
        gathered = lax.all_gather(activations, ("row", "col"), axis=1, tiled=True)
        gate_grad, up_grad = geglu_grads(gate_input, up_input, hidden_grad)
        gate_steps = reduce_tokens(gathered, gate_grad, 1)
        up_steps = reduce_tokens(gathered, up_grad, -1)
        input_grad = reduce_hidden(gate_grad, up_grad, weight_gate, weight_up)
        gate_part, up_part = next(gate_steps), next(up_steps)
        if outer == 4:
            gate_part, up_part, input_grad = lax.optimization_barrier(
                (gate_part, up_part, input_grad)
            )
            gate_part, up_part = gate_steps.send(gate_part), up_steps.send(up_part)
            gate_part, up_part = lax.optimization_barrier((gate_part, up_part))
            gate_part, up_part = gate_steps.send(gate_part), up_steps.send(up_part)
        gate_steps, up_steps = spread_tokens(gate_part, 1), spread_tokens(up_part, -1)
        gate_weight_grad, up_weight_grad = next(gate_steps), next(up_steps)
        for _ in range(2 if outer == 4 else 0):
            gate_weight_grad, up_weight_grad = lax.optimization_barrier(
                (gate_weight_grad, up_weight_grad)
            )
            gate_weight_grad = gate_steps.send(gate_weight_grad)
            up_weight_grad = up_steps.send(up_weight_grad)
        return (input_grad, gate_weight_grad, up_weight_grad)

    return body


def solution(mesh):
    in_specs = (
        P("dp", ("row", "col")),
        P("dp", ("row", "col")),
        P("dp", ("row", "col")),
        P("dp", ("row", "col")),
        P(None, ("row", "col")),
        P(None, ("row", "col")),
    )
    out_specs = (P("dp", ("row", "col")), P(None, ("row", "col")), P(None, ("row", "col")))
    body = make_body(mesh.shape["dp"], mesh.shape["row"], mesh.shape["col"])
    return jax.shard_map(body, mesh=mesh, in_specs=in_specs, out_specs=out_specs, check_vma=False)
```
